32 devices in a mesh: row: 16 (over z, y, x), col: 2 (over core).
Axes of the slice: x: 2, y: 2, z: 4, core: 2. Of those that a mesh axis runs over, the one named last changes fastest.
Arguments:
- top_tensor: bfloat16 [2304, 2304], P('row', 'col'), may hold values from -3 to 3
- bottom_tensor: bfloat16 [2304, 2304], P(('col', 'row')), may hold values from -3 to 3
- left_proj: bfloat16 [2304, 48], replicated, may hold values from -0.125 to 0.125
- right_proj: bfloat16 [2304, 48], replicated, may hold values from -0.125 to 0.125
Outputs:
- coarse: bfloat16 [2304, 2304], P(('col', 'row'))
The draws below stay inside these ranges and needn't reach their ends.
All inputs are finite; a program needn't handle non-finite values.
Results may differ from the reference program's by a relative error of at most 0.0065.
Values may be sent and summed in bfloat16 or wider, within the bound.
No kernel may reach another device: no remote copies, remote signals or barrier semaphores. Data moves between devices by JAX's collectives and lax.ppermute only.
A program may use at most 128 MiB of HBM per device.

```python
import jax
import jax.numpy as jnp
from jax import lax

CHI = 48
N_COL = 2


def block_scale(stream_key, shape, pieces, smallest, largest):
    def one(dim, shards_of):
        heights = jax.random.uniform(jax.random.fold_in(jax.random.fold_in(stream_key, 6), dim), (shards_of,), jnp.float32, smallest / len(pieces), largest / len(pieces))
        return jnp.repeat(jnp.exp(heights), shape[dim] // shards_of).reshape((-1,) + (1,) * (len(shape) - dim - 1))

    level = one(*pieces[0])
    for cut in pieces[1:]:
        level = level * one(*cut)
    return level


def bell_draw(stream_key, shape, spread, limit, pieces=(), kind=jnp.bfloat16):
    result = jax.random.normal(stream_key, shape, jnp.float32) * spread
    if len(pieces) > 0:
        result = block_scale(stream_key, shape, pieces, -0.22, 0.18) * result
    return jnp.clip(result, min=-limit, max=limit).astype(kind)


def setup_inputs(seed: int = 0) -> dict:
    keys = jax.random.split(jax.random.key(seed), 5)
    return {
        "top_tensor": bell_draw(keys[0], (CHI * CHI, CHI * CHI), 0.38, 3.0, ((0, 16), (1, 2))),
        "bottom_tensor": bell_draw(keys[1], (CHI * CHI, CHI * CHI), 0.38, 3.0, ((0, 32),)),
        "left_proj": bell_draw(keys[2], (CHI * CHI, CHI), (CHI * CHI) ** -0.5, 0.125),
        "right_proj": bell_draw(keys[3], (CHI * CHI, CHI), (CHI * CHI) ** -0.5, 0.125),
    }


def reference(top_tensor, bottom_tensor, left_proj, right_proj):
    bond_dim = CHI
    block_len = CHI // N_COL
    left_table = left_proj.reshape(bond_dim, bond_dim, bond_dim).astype(jnp.float32)
    upper_part = top_tensor.reshape(bond_dim, bond_dim, bond_dim, bond_dim)

    def one_up(upper_slice):
        weighted = jnp.einsum("rml,lka->ramk", upper_slice.astype(jnp.float32), left_table, precision=lax.Precision.HIGHEST)
        weighted = weighted.astype(jnp.bfloat16).reshape(bond_dim * bond_dim, bond_dim * bond_dim)
        running = jnp.zeros((bond_dim * bond_dim, bond_dim), jnp.float32)
        for block_idx in range(N_COL):
            first = block_idx * block_len * bond_dim
            last = first + block_len * bond_dim
            paired = jnp.dot(weighted[:, first:last], bottom_tensor[first:last], preferred_element_type=jnp.float32)
            paired = paired.astype(jnp.bfloat16).reshape(bond_dim, bond_dim, bond_dim, bond_dim)
            paired = paired.transpose(1, 2, 0, 3).reshape(bond_dim * bond_dim, bond_dim * bond_dim)
            running = running + jnp.dot(paired, right_proj, preferred_element_type=jnp.float32)
        return running.reshape(bond_dim, bond_dim, bond_dim)

    per_up = lax.map(one_up, upper_part)
    coarse = per_up.transpose(2, 1, 0, 3).reshape(bond_dim * bond_dim, bond_dim * bond_dim)
    return coarse.astype(jnp.bfloat16)
```

```python
import functools

import jax
import jax.numpy as jnp
from jax import lax
from jax.experimental import pallas as pl
from jax.experimental.pallas import tpu as pltpu
from jax.sharding import PartitionSpec as P

LANES = 256
ROW_TILE = 16
TURN = 128


def place_rows(arrived, window, rows_here, bond_dim, row_count):
    slot_ids = jnp.arange(row_count * window, dtype=jnp.int32)
    source_dev = slot_ids // window
    target_upper = source_dev * rows_here // bond_dim + slot_ids % window
    placing = (target_upper[:, None] == jnp.arange(bond_dim, dtype=jnp.int32)[None, :]).astype(
        jnp.float32
    )
    return jnp.einsum("rsb,su->rub", arrived, placing, precision=lax.Precision.HIGHEST)


def local_general(top_tensor, bottom_tensor, left_proj, right_proj):
    bond_dim = right_proj.shape[1]
    rows_here = top_tensor.shape[0]
    block_len = top_tensor.shape[1] // bond_dim
    lower_rows = lax.all_gather(bottom_tensor, "row", axis=0, tiled=True)
    left_table = left_proj.reshape(bond_dim, bond_dim, bond_dim)
    upper_part = top_tensor.reshape(rows_here, block_len, bond_dim)
    weighted = jnp.einsum(
        "rml,lka->ramk", upper_part, left_table, preferred_element_type=jnp.float32
    )
    weighted = weighted.astype(jnp.bfloat16).reshape(rows_here * bond_dim, block_len * bond_dim)
    window = rows_here // bond_dim + 2
    row_count = lax.axis_size("row")
    start_row = lax.axis_index("row") * rows_here
    first_upper = start_row // bond_dim
    offset_rows = start_row - first_upper * bond_dim
    group_size = 8
    groups = bond_dim // group_size
    column_sets = lower_rows.reshape(block_len * bond_dim, groups, group_size * bond_dim).transpose(
        1, 0, 2
    )

    def one_group(columns):
        product_part = jnp.dot(weighted, columns, preferred_element_type=jnp.float32).astype(
            jnp.bfloat16
        )
        product_part = product_part.reshape(rows_here, bond_dim, group_size, bond_dim)
        padded = jnp.zeros((window * bond_dim, bond_dim, group_size, bond_dim), jnp.bfloat16)
        padded = lax.dynamic_update_slice_in_dim(padded, product_part, offset_rows, 0)
        regrid = padded.reshape(window, bond_dim, bond_dim, group_size, bond_dim).transpose(
            0, 2, 3, 1, 4
        )
        regrid = regrid.reshape(window * bond_dim * group_size, bond_dim * bond_dim)
        projected = jnp.dot(regrid, right_proj, preferred_element_type=jnp.float32)
        return projected.reshape(window, bond_dim, group_size, bond_dim)

    stacked = lax.map(one_group, column_sets)
    per_down = stacked.transpose(0, 3, 2, 1, 4).reshape(bond_dim, bond_dim, window, bond_dim)
    summed = lax.psum_scatter(per_down, "col", scatter_dimension=0, tiled=True)
    summed = summed.reshape(summed.shape[0] * bond_dim, window, bond_dim)
    arrived = lax.all_to_all(summed, "row", split_axis=0, concat_axis=1, tiled=True)
    combined = place_rows(arrived, window, rows_here, bond_dim, row_count)
    out_rows = combined.shape[0]
    return combined.reshape(out_rows, bond_dim * bond_dim).astype(jnp.bfloat16)


def spread_diagonal(tile, copies):
    size = tile.shape[0]
    lane = lax.broadcasted_iota(jnp.int32, tile.shape, 1)
    parts = [
        jnp.where((lane >= k * size) & (lane < (k + 1) * size), tile, jnp.zeros_like(tile))
        for k in range(copies)
    ]
    if LANES > copies * size:
        parts.append(jnp.zeros((LANES - copies * size, LANES), tile.dtype))
    return jnp.concatenate(parts, axis=0)


def kernel_body(bond_dim, downs, packs, copies, n_lower, *refs):
    lower_refs = refs[:n_lower]
    upper_ref, left_ref, right_ref, out_ref = refs[n_lower : n_lower + 4]
    turned_ref, weight_ref, product_ref, paired_ref, diag_ref = refs[n_lower + 4 :]

    @pl.when(pl.program_id(0) == 0)
    def _():
        at = 0
        for ref in lower_refs:
            for first in range(0, ref.shape[0], TURN):
                turned_ref[:, at : at + TURN] = ref[first : first + TURN, :].T
                at += TURN

        def fill(k, carry):
            diag_ref[pl.ds(pl.multiple_of(k * LANES, LANES), LANES), :] = spread_diagonal(right_ref[k], copies)
            return carry

        lax.fori_loop(0, bond_dim, fill, 0)

    def weigh(m, carry):
        mixed = jnp.dot(
            left_ref[...], spread_diagonal(upper_ref[0, m], copies), preferred_element_type=jnp.float32
        ).astype(jnp.bfloat16)
        rows = pl.ds(pl.multiple_of(m * bond_dim, bond_dim), bond_dim)
        for g in range(packs):
            weight_ref[g // 2, rows, (g % 2) * LANES : (g % 2 + 1) * LANES] = mixed[
                g * bond_dim : (g + 1) * bond_dim
            ]
        return carry

    lax.fori_loop(0, bond_dim, weigh, 0)

    def multiply(pair, carry):
        product_ref[...] = jnp.dot(
            turned_ref[...], weight_ref[pair], preferred_element_type=jnp.float32
        )
        rows = pl.ds(pl.multiple_of(pair * 2 * downs, ROW_TILE), 2 * downs)
        for k in range(bond_dim):
            part = product_ref[k * downs : (k + 1) * downs, :]
            both = jnp.concatenate([part[:, :LANES], part[:, LANES:]], axis=0)
            paired_ref[rows, k * LANES : (k + 1) * LANES] = both.astype(jnp.bfloat16)
        return carry

    lax.fori_loop(0, packs // 2, multiply, 0)
    out_ref[0] = jnp.dot(
        paired_ref[...], diag_ref[...], preferred_element_type=jnp.float32
    ).astype(jnp.bfloat16)


def local_aligned(top_tensor, bottom_tensor, left_proj, right_proj):
    bond_dim = right_proj.shape[1]
    uppers = top_tensor.shape[0] // bond_dim
    n_col = lax.axis_size("col")
    downs = bond_dim // n_col
    copies = LANES // bond_dim
    packs = -(-bond_dim // copies)
    packs += packs % 2
    spare = LANES - copies * bond_dim

    lower_rows = bottom_tensor.shape[0]
    lower = bottom_tensor.reshape(lower_rows, n_col, downs, bond_dim).transpose(1, 0, 3, 2)
    lower = lower.reshape(n_col, lower_rows, bond_dim * downs)
    lower = lax.all_to_all(lower, "col", split_axis=0, concat_axis=0, tiled=True)
    lowers = [lax.all_gather(lower[c], "row", axis=0, tiled=True) for c in range(n_col)]

    upper = lax.all_gather(top_tensor, "col", axis=1, tiled=True)
    upper = upper.reshape(uppers, bond_dim, bond_dim, bond_dim).transpose(0, 2, 3, 1)
    upper = jnp.pad(jnp.tile(upper, (1, 1, 1, copies)), ((0, 0), (0, 0), (0, 0), (0, spare)))

    left = left_proj.reshape(bond_dim, bond_dim, bond_dim).transpose(2, 1, 0)
    left = jnp.pad(left, ((0, packs * copies - bond_dim), (0, 0), (0, 0)))
    left = left.reshape(packs, copies, bond_dim, bond_dim).transpose(0, 2, 1, 3)
    left = jnp.pad(
        left.reshape(packs * bond_dim, copies * bond_dim), ((0, 0), (0, spare))
    )

    right = right_proj.reshape(bond_dim, bond_dim, bond_dim).transpose(1, 0, 2)
    right = jnp.pad(jnp.tile(right, (1, 1, copies)), ((0, 0), (0, 0), (0, spare)))

    inner = bond_dim * bond_dim
    whole = lambda shape: pl.BlockSpec(
        shape, lambda u: (0,) * len(shape), pipeline_mode=pl.Buffered(1)
    )
    result = pl.pallas_call(
        functools.partial(kernel_body, bond_dim, downs, packs, copies, n_col),
        grid=(uppers,),
        in_specs=[whole(x.shape) for x in lowers]
        + [
            pl.BlockSpec((1, bond_dim, bond_dim, LANES), lambda u: (u, 0, 0, 0)),
            whole(left.shape),
            whole(right.shape),
        ],
        out_specs=pl.BlockSpec((1, packs * downs, LANES), lambda u: (u, 0, 0)),
        out_shape=jax.ShapeDtypeStruct((uppers, packs * downs, LANES), jnp.bfloat16),
        scratch_shapes=[
            pltpu.VMEM((bond_dim * downs, inner), jnp.bfloat16),
            pltpu.VMEM((packs // 2, inner, 2 * LANES), jnp.bfloat16),
            pltpu.VMEM((bond_dim * downs, 2 * LANES), jnp.float32),
            pltpu.VMEM((packs * downs, bond_dim * LANES), jnp.bfloat16),
            pltpu.VMEM((bond_dim * LANES, LANES), jnp.bfloat16),
        ],
        compiler_params=pltpu.CompilerParams(
            dimension_semantics=("arbitrary",), vmem_limit_bytes=58 * 1024 * 1024
        ),
    )(*lowers, upper, left, right)

    result = result.reshape(uppers, packs, downs, LANES)[..., : copies * bond_dim]
    result = result.reshape(uppers, packs, downs, copies, bond_dim).transpose(2, 1, 3, 0, 4)
    result = result.reshape(downs, packs * copies, uppers * bond_dim)[:, :bond_dim]
    result = result.reshape(downs * bond_dim, uppers * bond_dim)
    return lax.all_to_all(result, "row", split_axis=0, concat_axis=1, tiled=True)


def local(top_tensor, bottom_tensor, left_proj, right_proj):
    bond_dim = right_proj.shape[1]
    n_col = lax.axis_size("col")
    aligned = (
        top_tensor.shape[0] % bond_dim == 0
        and bond_dim % n_col == 0
        and (bond_dim // n_col) % 8 == 0
        and bond_dim % ROW_TILE == 0
        and bottom_tensor.shape[0] * lax.axis_size("row") % TURN == 0
    )
    route = local_aligned if aligned else local_general
    return route(top_tensor, bottom_tensor, left_proj, right_proj)


def solution(mesh):
    return jax.shard_map(
        local,
        mesh=mesh,
        in_specs=(P("row", "col"), P(("col", "row"), None), P(), P()),
        out_specs=P(("col", "row"), None),
        check_vma=False,
    )
```

```python
import functools

import jax
import jax.numpy as jnp
from jax import lax
from jax.experimental import pallas as pl
from jax.experimental.pallas import tpu as pltpu
from jax.sharding import PartitionSpec as P

LANES = 256
ROW_TILE = 16
TURN = 128


def place_rows(arrived, window, rows_here, bond_dim, row_count):
    slot_ids = jnp.arange(row_count * window, dtype=jnp.int32)
    source_dev = slot_ids // window
    target_upper = source_dev * rows_here // bond_dim + slot_ids % window
    placing = (target_upper[:, None] == jnp.arange(bond_dim, dtype=jnp.int32)[None, :]).astype(
        jnp.float32
    )
    return jnp.einsum("rsb,su->rub", arrived, placing, precision=lax.Precision.HIGHEST)


def local_general(top_tensor, bottom_tensor, left_proj, right_proj):
    bond_dim = right_proj.shape[1]
    rows_here = top_tensor.shape[0]
    block_len = top_tensor.shape[1] // bond_dim
    lower_rows = lax.all_gather(bottom_tensor, "row", axis=0, tiled=True)
    left_table = left_proj.reshape(bond_dim, bond_dim, bond_dim)
    upper_part = top_tensor.reshape(rows_here, block_len, bond_dim)
    weighted = jnp.einsum(
        "rml,lka->ramk", upper_part, left_table, preferred_element_type=jnp.float32
    )
    weighted = weighted.astype(jnp.bfloat16).reshape(rows_here * bond_dim, block_len * bond_dim)
    window = rows_here // bond_dim + 2
    row_count = lax.axis_size("row")
    start_row = lax.axis_index("row") * rows_here
    first_upper = start_row // bond_dim
    offset_rows = start_row - first_upper * bond_dim
    group_size = 8
    groups = bond_dim // group_size
    column_sets = lower_rows.reshape(block_len * bond_dim, groups, group_size * bond_dim).transpose(
        1, 0, 2
    )

    def one_group(columns):
        product_part = jnp.dot(weighted, columns, preferred_element_type=jnp.float32).astype(
            jnp.bfloat16
        )
        product_part = product_part.reshape(rows_here, bond_dim, group_size, bond_dim)
        padded = jnp.zeros((window * bond_dim, bond_dim, group_size, bond_dim), jnp.bfloat16)
        padded = lax.dynamic_update_slice_in_dim(padded, product_part, offset_rows, 0)
        regrid = padded.reshape(window, bond_dim, bond_dim, group_size, bond_dim).transpose(
            0, 2, 3, 1, 4
        )
        regrid = regrid.reshape(window * bond_dim * group_size, bond_dim * bond_dim)
        projected = jnp.dot(regrid, right_proj, preferred_element_type=jnp.float32)
        return projected.reshape(window, bond_dim, group_size, bond_dim)

    stacked = lax.map(one_group, column_sets)
    per_down = stacked.transpose(0, 3, 2, 1, 4).reshape(bond_dim, bond_dim, window, bond_dim)
    summed = lax.psum_scatter(per_down, "col", scatter_dimension=0, tiled=True)
    summed = summed.reshape(summed.shape[0] * bond_dim, window, bond_dim)
    arrived = lax.all_to_all(summed, "row", split_axis=0, concat_axis=1, tiled=True)
    combined = place_rows(arrived, window, rows_here, bond_dim, row_count)
    out_rows = combined.shape[0]
    return combined.reshape(out_rows, bond_dim * bond_dim).astype(jnp.bfloat16)


def spread_diagonal(tile, copies):
    size = tile.shape[0]
    lane = lax.broadcasted_iota(jnp.int32, tile.shape, 1)
    parts = [
        jnp.where((lane >= k * size) & (lane < (k + 1) * size), tile, jnp.zeros_like(tile))
        for k in range(copies)
    ]
    if LANES > copies * size:
        parts.append(jnp.zeros((LANES - copies * size, LANES), tile.dtype))
    return jnp.concatenate(parts, axis=0)


def kernel_body(bond_dim, downs, packs, copies, n_lower, *refs):
    lower_refs = refs[:n_lower]
    upper_ref, left_ref, right_ref, out_ref = refs[n_lower : n_lower + 4]
    turned_ref, weight_ref, product_ref, paired_ref, diag_ref = refs[n_lower + 4 :]

    @pl.when(pl.program_id(0) == 0)
    def _():
        at = 0
        for ref in lower_refs:
            for first in range(0, ref.shape[0], TURN):
                turned_ref[:, at : at + TURN] = ref[first : first + TURN, :].T
                at += TURN

        def fill(k, carry):
            diag_ref[pl.ds(pl.multiple_of(k * LANES, LANES), LANES), :] = spread_diagonal(right_ref[k], copies)
            return carry

        lax.fori_loop(0, bond_dim, fill, 0)

    def weigh(m, carry):
        mixed = jnp.dot(
            left_ref[...], spread_diagonal(upper_ref[0, m], copies), preferred_element_type=jnp.float32
        ).astype(jnp.bfloat16)
        rows = pl.ds(pl.multiple_of(m * bond_dim, bond_dim), bond_dim)
        for g in range(packs):
            weight_ref[g // 2, rows, (g % 2) * LANES : (g % 2 + 1) * LANES] = mixed[
                g * bond_dim : (g + 1) * bond_dim
            ]
        return carry

    lax.fori_loop(0, bond_dim, weigh, 0)

    def multiply(pair, carry):
        product_ref[...] = jnp.dot(
            turned_ref[...], weight_ref[pair], preferred_element_type=jnp.float32
        )
        rows = pl.ds(pl.multiple_of(pair * 2 * downs, ROW_TILE), 2 * downs)
        for k in range(bond_dim):
            part = product_ref[k * downs : (k + 1) * downs, :]
            both = jnp.concatenate([part[:, :LANES], part[:, LANES:]], axis=0)
            paired_ref[rows, k * LANES : (k + 1) * LANES] = both.astype(jnp.bfloat16)
        return carry

    lax.fori_loop(0, packs // 2, multiply, 0)
    out_ref[0] = jnp.dot(
        paired_ref[...], diag_ref[...], preferred_element_type=jnp.float32
    ).astype(jnp.bfloat16)


def direct_gather(shard, axis):
    count = lax.axis_size(axis)
    here = lax.axis_index(axis)
    rows = shard.shape[0]
    paired = count & (count - 1) == 0
    send = (lambda r, k: r ^ k) if paired else (lambda r, k: (r + k) % count)
    origin = (lambda r, k: r ^ k) if paired else (lambda r, k: (r - k) % count)
    pieces = [
        lax.ppermute(shard, axis, [(r, send(r, k)) for r in range(count)]) for k in range(1, count)
    ]
    gathered = jnp.zeros((count * rows,) + shard.shape[1:], shard.dtype)
    for k, piece in enumerate([shard] + pieces):
        gathered = lax.dynamic_update_slice_in_dim(gathered, piece, origin(here, k) * rows, 0)
    return gathered


def local_aligned(top_tensor, bottom_tensor, left_proj, right_proj):
    bond_dim = right_proj.shape[1]
    uppers = top_tensor.shape[0] // bond_dim
    n_col = lax.axis_size("col")
    downs = bond_dim // n_col
    copies = LANES // bond_dim
    packs = -(-bond_dim // copies)
    packs += packs % 2
    spare = LANES - copies * bond_dim

    lower_rows = bottom_tensor.shape[0]
    lower = bottom_tensor.reshape(lower_rows, n_col, downs, bond_dim).transpose(1, 0, 3, 2)
    lower = lower.reshape(n_col, lower_rows, bond_dim * downs)
    lower = lax.all_to_all(lower, "col", split_axis=0, concat_axis=0, tiled=True)
    lowers = [
        direct_gather(lower[c], "row") if c % 2 else lax.all_gather(lower[c], "row", axis=0, tiled=True)
        for c in range(n_col)
    ]

    upper = lax.all_gather(top_tensor, "col", axis=1, tiled=True)
    upper = upper.reshape(uppers, bond_dim, bond_dim, bond_dim).transpose(0, 2, 3, 1)
    upper = jnp.pad(jnp.tile(upper, (1, 1, 1, copies)), ((0, 0), (0, 0), (0, 0), (0, spare)))

    left = left_proj.reshape(bond_dim, bond_dim, bond_dim).transpose(2, 1, 0)
    left = jnp.pad(left, ((0, packs * copies - bond_dim), (0, 0), (0, 0)))
    left = left.reshape(packs, copies, bond_dim, bond_dim).transpose(0, 2, 1, 3)
    left = jnp.pad(
        left.reshape(packs * bond_dim, copies * bond_dim), ((0, 0), (0, spare))
    )

    right = right_proj.reshape(bond_dim, bond_dim, bond_dim).transpose(1, 0, 2)
    right = jnp.pad(jnp.tile(right, (1, 1, copies)), ((0, 0), (0, 0), (0, spare)))

    inner = bond_dim * bond_dim
    whole = lambda shape: pl.BlockSpec(
        shape, lambda u: (0,) * len(shape), pipeline_mode=pl.Buffered(1)
    )
    result = pl.pallas_call(
        functools.partial(kernel_body, bond_dim, downs, packs, copies, n_col),
        grid=(uppers,),
        in_specs=[whole(x.shape) for x in lowers]
        + [
            pl.BlockSpec((1, bond_dim, bond_dim, LANES), lambda u: (u, 0, 0, 0)),
            whole(left.shape),
            whole(right.shape),
        ],
        out_specs=pl.BlockSpec((1, packs * downs, LANES), lambda u: (u, 0, 0)),
        out_shape=jax.ShapeDtypeStruct((uppers, packs * downs, LANES), jnp.bfloat16),
        scratch_shapes=[
            pltpu.VMEM((bond_dim * downs, inner), jnp.bfloat16),
            pltpu.VMEM((packs // 2, inner, 2 * LANES), jnp.bfloat16),
            pltpu.VMEM((bond_dim * downs, 2 * LANES), jnp.float32),
            pltpu.VMEM((packs * downs, bond_dim * LANES), jnp.bfloat16),
            pltpu.VMEM((bond_dim * LANES, LANES), jnp.bfloat16),
        ],
        compiler_params=pltpu.CompilerParams(
            dimension_semantics=("arbitrary",), vmem_limit_bytes=58 * 1024 * 1024
        ),
    )(*lowers, upper, left, right)

    result = result.reshape(uppers, packs, downs, LANES)[..., : copies * bond_dim]
    result = result.reshape(uppers, packs, downs, copies, bond_dim).transpose(2, 1, 3, 0, 4)
    result = result.reshape(downs, packs * copies, uppers * bond_dim)[:, :bond_dim]
    result = result.reshape(downs * bond_dim, uppers * bond_dim)
    return lax.all_to_all(result, "row", split_axis=0, concat_axis=1, tiled=True)


def local(top_tensor, bottom_tensor, left_proj, right_proj):
    bond_dim = right_proj.shape[1]
    n_col = lax.axis_size("col")
    aligned = (
        top_tensor.shape[0] % bond_dim == 0
        and bond_dim % n_col == 0
        and (bond_dim // n_col) % 8 == 0
        and bond_dim % ROW_TILE == 0
        and bottom_tensor.shape[0] * lax.axis_size("row") % TURN == 0
    )
    route = local_aligned if aligned else local_general
    return route(top_tensor, bottom_tensor, left_proj, right_proj)


def solution(mesh):
    return jax.shard_map(
        local,
        mesh=mesh,
        in_specs=(P("row", "col"), P(("col", "row"), None), P(), P()),
        out_specs=P(("col", "row"), None),
        check_vma=False,
    )
```
